128 devices in a mesh: dp: 16 (over y, z_hi, core), mp: 8 (over z_lo, x).
Axes of the slice: x: 4, y: 4, z: 4 (z_hi: 2, z_lo: 2; z = z_hi * 2 + z_lo), core: 2. Of those that a mesh axis runs over, the one named last changes fastest.
Arguments:
- attn_out: bfloat16 [16384, 8192], P('dp', 'mp'), may hold values from -6 to 6
- out_weight: bfloat16 [8192, 8192], P('dp'), may hold values from -0.09375 to 0.09375
- residual: bfloat16 [16, 1024, 8192], P(None, 'mp', 'dp'), may hold values from -6 to 6
Outputs:
- layer_out: bfloat16 [16, 1024, 8192], P(None, 'mp', 'dp')
The draws below stay inside these ranges and needn't reach their ends.
All inputs are finite; a program needn't handle non-finite values.
Results may differ from the reference program's by a relative error of at most 0.001.
Values may be sent and summed in bfloat16 or wider, within the bound.
No kernel may reach another device: no remote copies, remote signals or barrier semaphores. Data moves between devices by JAX's collectives and lax.ppermute only.
A program may use at most 192 MiB of HBM per device.

```python
import jax
import jax.numpy as jnp

D = 8192
TOK_DEV = 1024
HD = 8192
TOKENS = 16384
N_DP = 16


def with_spikes(array, stream_key, source, target, parts, factor):
    owner, partner = [(jnp.arange(array.shape[position]) // (array.shape[position] // parts)).reshape([-1 if axis == position else 1 for axis in range(array.ndim)]) for position in (source, target)]
    chosen = jax.random.permutation(stream_key, parts)[partner]
    strong = (owner == chosen) | (owner == (partner + parts // 2) % parts)
    return jnp.where(strong, factor * array, array)


def steps_of(stream_key, dims, pieces, least, high):
    def one(position, blocks):
        draws = jax.random.uniform(jax.random.fold_in(jax.random.fold_in(stream_key, 6), position), (blocks,), jnp.float32, least / len(pieces), high / len(pieces))
        return jnp.repeat(jnp.exp(draws), dims[position] // blocks).reshape((-1,) + (1,) * (len(dims) - position - 1))

    factor_of = one(*pieces[0])
    for cut in pieces[1:]:
        factor_of = factor_of * one(*cut)
    return factor_of


def bell_draw(key, dims, spread, reach, pieces=(), dtype=jnp.bfloat16):
    level = steps_of(key, dims, pieces, -0.22, 0.18) if pieces else 1.0
    entries = jax.random.normal(key, dims, jnp.float32) * spread * level
    return jnp.minimum(jnp.maximum(entries, -reach), reach).astype(dtype)


def noise_with(key, dims, scale, limit, split, heavy, held_as=jnp.bfloat16):
    entries = scale * jax.random.normal(key, dims, jnp.float32)
    if split:
        entries = entries * steps_of(key, dims, split, -0.22, 0.18)
    return jnp.clip(with_spikes(entries, jax.random.fold_in(key, 3), *heavy), -limit, limit).astype(held_as)


def setup_inputs(seed: int = 0) -> dict:
    splits = jax.random.split(jax.random.key(seed), 4)
    attn_out = bell_draw(splits[0], (TOKENS, HD), 1.0, 6.0, ((0, 16), (1, 8)))
    out_weight = noise_with(splits[1], (HD, D), HD ** -0.5, 0.09375, ((0, 16),), (0, 1, 16, 2.0))
    residual = bell_draw(splits[2], (N_DP, TOK_DEV, D), 1.0, 6.0, ((1, 8), (2, 16)))
    return {"attn_out": attn_out, "out_weight": out_weight, "residual": residual}


def reference(attn_out, out_weight, residual):
    projected = jnp.dot(attn_out, out_weight, preferred_element_type=jnp.float32)
    projected = projected.reshape(N_DP, TOK_DEV, D)
    return (residual.astype(jnp.float32) + projected).astype(jnp.bfloat16)
```

```python
import itertools

import jax
import jax.numpy as jnp
from jax import lax
from jax.sharding import Mesh
from jax.sharding import PartitionSpec as P

AXES = ("y", "zh", "c", "zl", "x")
SIZES = (4, 2, 2, 2, 4)
Z = ("zh", "zl")
PART = 255.0 / 1152.0
FULL = 255.0 / 4608.0


def flat(coords):
    index = 0
    for coord, size in zip(coords, SIZES):
        index = index * size + coord
    return index


def moves(target):
    return [
        (flat(s), flat(target(*s)))
        for s in itertools.product(*(range(n) for n in SIZES))
    ]


def ring(shift):
    return [(i, (i + shift) % 4) for i in range(4)]


PARTNER = [(0, 1), (1, 0), (2, 3), (3, 2)]
OTHER = [(1, 2), (2, 1), (3, 0), (0, 3)]
CORES = [(0, 1), (1, 0)]


def code(value, scale):
    value = value * scale
    return (value * jnp.abs(value)).astype(jnp.float16)


def decode(coded, scale):
    coded = coded.astype(jnp.float32)
    root = jnp.sqrt(jnp.abs(coded)) * (1.0 / scale)
    return jnp.where(coded < 0, -root, root)


def pick(array, index, axis=0):
    return lax.dynamic_index_in_dim(array, index, axis, keepdims=False)


def shards(attn, weight, residual):
    y, zh, c, zl, x = (lax.axis_index(a) for a in AXES)

    own_1 = lax.ppermute(attn, Z, PARTNER)
    oth_1 = lax.ppermute(attn, Z, OTHER)
    low = lax.ppermute(oth_1[:512], Z, PARTNER)
    high = lax.ppermute(own_1[512:], Z, OTHER)

    blocks = weight.reshape(512, 2, 2, 4, 512)
    piece = lax.dynamic_slice(
        blocks, (0, x & 1, 0, (x >> 1) * 2 + zl, 0), (512, 1, 2, 1, 512)
    ).reshape(512, 2, 512)
    piece = lax.ppermute(
        piece.reshape(512, 1024),
        AXES,
        moves(
            lambda y, zh, c, zl, x: (
                (y & 2) | (x & 1), x >> 1, c, zl, ((y & 1) << 1) | zh,
            )
        ),
    )
    cols = jnp.zeros((2, 4, 1024, 512), weight.dtype)
    for shift in range(4):
        got = piece if shift == 0 else lax.ppermute(piece, "y", ring(shift))
        twin = lax.ppermute(got, "c", CORES)
        src = (y - shift) % 4
        k = (src >> 1) ^ zl
        for core, part in ((c, got), (1 - c, twin)):
            for y0 in range(2):
                dy = ((src & 1) * 2 + y0 - y) % 4
                cols = lax.dynamic_update_slice(
                    cols,
                    part[None, None, :, y0 * 512 : y0 * 512 + 512],
                    (k, dy, core * 512, 0),
                )

    oth_0 = jnp.concatenate([low, high], axis=0)
    out = residual
    for other, dy in itertools.product(range(2), (0, 2, 1, 3)):
        a0, a1 = (oth_0, oth_1) if other else (attn, own_1)
        part = jnp.dot(a0, cols[0, dy], preferred_element_type=jnp.float32)
        part += jnp.dot(a1, cols[1, dy], preferred_element_type=jnp.float32)
        part = part.reshape(2, 4, 128, 512)
        total = pick(part, x, 1)
        for shift in range(1, 4):
            sent = code(pick(part, (x + shift) % 4, 1), PART)
            total += decode(lax.ppermute(sent, "x", ring(shift)), PART)
        total = code(total, FULL)
        for j in range(2):
            got = lax.ppermute(
                pick(total, c ^ j),
                AXES,
                moves(lambda y, zh, c, zl, x: ((y + dy) % 4, zh, zl, c ^ j, x)),
            )
            i = ((y - dy) % 4) * 4 + (zh ^ other) * 2 + (zl ^ j)
            new = pick(residual, i).astype(jnp.float32)
            new += decode(got, FULL)
            out = lax.dynamic_update_index_in_dim(
                out, new.astype(out.dtype), i, 0
            )
    return out


def solution(mesh):
    torus = Mesh(mesh.devices.reshape(SIZES), AXES)
    return jax.shard_map(
        shards,
        mesh=torus,
        in_specs=(
            P(("y", "zh", "c"), ("zl", "x")),
            P(("y", "zh", "c"), None),
            P(None, ("zl", "x"), ("y", "zh", "c")),
        ),
        out_specs=P(None, ("zl", "x"), ("y", "zh", "c")),
        check_vma=False,
    )
```

```python
import functools
import itertools

import jax
import jax.numpy as jnp
from jax import lax
from jax.experimental import pallas as pl
from jax.experimental.pallas import tpu as pltpu
from jax.sharding import Mesh
from jax.sharding import PartitionSpec as P

AXES = ("y", "zh", "c", "zl", "x")
SIZES = (4, 2, 2, 2, 4)
Z = ("zh", "zl")
BF16, F32 = jnp.bfloat16, jnp.float32


PART = (0.03, 4.6)
FULL = (0.12, 18.4)


def code(value, scale):
    floor, unit = scale
    power = (jnp.abs(value) + floor) * (1.0 / unit)
    for _ in range(4):
        power = power * power
    return jnp.where(value < 0, -power, power).astype(BF16)


def decode(coded, scale):
    floor, unit = scale
    coded = coded.astype(F32)
    value = jnp.exp(jnp.log(jnp.abs(coded)) * 0.0625) * unit - floor
    return jnp.where(coded < 0, -value, value)


def flat(coords):
    index = 0
    for coord, size in zip(coords, SIZES):
        index = index * size + coord
    return index


def moves(target):
    return [
        (flat(s), flat(target(*s)))
        for s in itertools.product(*(range(n) for n in SIZES))
    ]


def ring(shift):
    return [(i, (i + shift) % 4) for i in range(4)]


PARTNER = [(0, 1), (1, 0), (2, 3), (3, 2)]
OTHER = [(1, 2), (2, 1), (3, 0), (0, 3)]
CORES = [(0, 1), (1, 0)]
PARAMS = pltpu.CompilerParams(vmem_limit_bytes=48 << 20)


def whole(shape):
    return pl.BlockSpec(shape, lambda *_: (0,) * len(shape))


def tile_body(n, parts, scalars, *refs):
    halves, refs = refs[: sum(parts)], refs[sum(parts) :]
    pieces, (own, *sent), rows = refs[: 2 * n], refs[2 * n : -1], refs[-1]
    step = pl.program_id(0)
    first = 0
    for k, count in enumerate(parts):
        for h in range(2):
            block = halves[first][h, 0] if count == 1 else halves[first + h][0]
            rows[h * 128 : h * 128 + 128, k * 1024 : k * 1024 + 1024] = block
        first += count
    core = scalars[1]
    for g in range(n):
        total = None
        for p, twin in itertools.product(range(2), range(2)):
            start = (scalars[2 + g] ^ p) * 1024 + (core ^ twin) * 512
            term = jnp.dot(
                rows[:, pl.ds(pl.multiple_of(start, 512), 512)],
                pieces[2 * g + twin][p],
                preferred_element_type=F32,
            )
            total = term if total is None else total + term
        total = total.reshape(2, 128, 512)
        span = slice(g * 512, g * 512 + 512)

        @pl.when(step == 0)
        def _():
            own[:, :, span] = total

        @pl.when(step > 0)
        def _():
            coded = code(total, PART)
            for k, ref in enumerate(sent):

                @pl.when(step == k + 1)
                def _():
                    ref[:, :, span] = coded


def tile(scalars, attn0, attn1, pieces):
    n = len(pieces)
    specs, operands = [], []
    for parts in (attn0, attn1):
        for part in parts:
            if len(parts) == 1:
                operands.append(part.reshape(2, 4, 128, 1024))
                specs.append(
                    pl.BlockSpec(
                        (2, 1, 128, 1024), lambda i, s: (0, (s[0] + i) % 4, 0, 0)
                    )
                )
            else:
                operands.append(part.reshape(4, 128, 1024))
                specs.append(
                    pl.BlockSpec((1, 128, 1024), lambda i, s: ((s[0] + i) % 4, 0, 0))
                )
    flat_pieces = [p for pair in pieces for p in pair]
    shape = (2, 128, 512 * n)
    return pl.pallas_call(
        functools.partial(tile_body, n, (len(attn0), len(attn1))),
        grid_spec=pltpu.PrefetchScalarGridSpec(
            num_scalar_prefetch=1,
            grid=(4,),
            in_specs=specs + [whole((2, 512, 512))] * (2 * n),
            out_specs=[whole(shape)] * 4,
            scratch_shapes=[pltpu.VMEM((256, 2048), BF16)],
        ),
        out_shape=[jax.ShapeDtypeStruct(shape, F32)]
        + [jax.ShapeDtypeStruct(shape, BF16)] * 3,
        compiler_params=PARAMS,
        cost_estimate=pl.CostEstimate(
            flops=n << 31, bytes_accessed=(6 + 3 * n) << 20, transcendentals=0
        ),
        name=f"tile{n}{len(attn0)}",
    )(scalars, *operands, *flat_pieces)


def reduced(own, got):
    total = own[...]
    for ref in got:
        total = total + decode(ref[...], PART)
    return code(total, FULL)


def collect_body(own, *refs):
    refs[-1][...] = reduced(own, refs[:-1])


def collect(own, got):
    shape = own.shape
    block = pl.BlockSpec((1, 128, 512), lambda i, j: (i, 0, j))
    return pl.pallas_call(
        collect_body,
        grid=(2, shape[2] // 512),
        in_specs=[block] * 4,
        out_specs=block,
        out_shape=jax.ShapeDtypeStruct(shape, BF16),
        compiler_params=PARAMS,
        cost_estimate=pl.CostEstimate(
            flops=shape[2] << 20, bytes_accessed=shape[2] << 12, transcendentals=0
        ),
        name="collect",
    )(own, *got)


def release_body(scalars, own, got1, got2, got3, first0, first1, *outs):
    j = pl.program_id(0)
    coded = reduced(own, (got1, got2, got3))
    for g, first in enumerate((first0, first1)):
        for k in range(2):

            @pl.when(j == k)
            def _():
                outs[2 * g + k][0] = first[0]
                outs[2 * g + k][1] = coded[0, :, g * 512 : g * 512 + 512]


def release(scalars, own, got, firsts):
    block = pl.BlockSpec((1, 128, 1024), lambda j, s: (s[1] ^ j, 0, 0))
    specs, operands = [], []
    for array, column in firsts:
        operands.append(array)
        specs.append(
            pl.BlockSpec((1, 128, 512), lambda j, s, q=column: (s[1] ^ j, 0, q))
        )
    shape = (2, 128, 512)
    return pl.pallas_call(
        release_body,
        grid_spec=pltpu.PrefetchScalarGridSpec(
            num_scalar_prefetch=1,
            grid=(2,),
            in_specs=[block] * 4 + specs,
            out_specs=[whole(shape)] * 4,
        ),
        out_shape=[jax.ShapeDtypeStruct(shape, BF16)] * 4,
        compiler_params=PARAMS,
        cost_estimate=pl.CostEstimate(
            flops=1 << 30, bytes_accessed=1 << 22, transcendentals=0
        ),
        name="release",
    )(scalars, own, *got, *operands)


def finish_body(scalars, *refs):
    gots, residual, out = refs[:4], refs[4], refs[-1]
    step = pl.program_id(0)
    for q, got in enumerate(gots):

        @pl.when(step >> 1 == q)
        def _():
            total = residual[0].astype(F32) + decode(got[step & 1], FULL)
            out[0] = total.astype(BF16)


def finish(places, gots, residual, partial):
    block = pl.BlockSpec((1, 128, 512), lambda t, s: (s[t], 0, 0))
    extra = [] if partial is None else [partial]
    return pl.pallas_call(
        finish_body,
        grid_spec=pltpu.PrefetchScalarGridSpec(
            num_scalar_prefetch=1,
            grid=(8,),
            in_specs=[whole((2, 128, 512))] * 4
            + [block]
            + [pl.BlockSpec(memory_space=pl.ANY)] * len(extra),
            out_specs=block,
        ),
        out_shape=jax.ShapeDtypeStruct(residual.shape, residual.dtype),
        input_output_aliases={6: 0} if extra else {},
        compiler_params=PARAMS,
        cost_estimate=pl.CostEstimate(
            flops=1 << 30, bytes_accessed=1 << 22, transcendentals=0
        ),
        name="finish",
    )(places, *gots, residual, *extra)


def shards(attn, weight, residual):
    y, zh, c, zl, x = (lax.axis_index(a) for a in AXES)

    piece = []
    for p in range(2):
        target = ((y >> 1) ^ p) * 8 + (x & 1) * 4 + (x >> 1) * 2 + zl
        sent = lax.dynamic_slice(weight, (0, target * 512), (512, 512))
        to = moves(
            lambda y, zh, c, zl, x: (
                ((y >> 1) ^ p) * 2 + (x & 1), x >> 1, c, zl, (y & 1) * 2 + zh,
            )
        )
        piece.append(lax.ppermute(sent, AXES, to))

    own_1 = lax.ppermute(attn, Z, PARTNER)
    oth_1 = lax.ppermute(attn, Z, OTHER)
    low = lax.ppermute(oth_1[:512], Z, PARTNER)
    high = lax.ppermute(own_1[512:], Z, OTHER)

    piece = jnp.stack(piece)
    pieces = {}
    for shift in (0, 1, 3, 2):
        got = piece if shift == 0 else lax.ppermute(piece, "y", ring(shift))
        pieces[shift] = (got, lax.ppermute(got, "c", CORES))

    def partials(attn0, attn1, shifts):
        base = [(((y - s) % 4) >> 1) ^ zl for s in shifts]
        own, *sent = tile(
            jnp.stack([x, c, *base]), attn0, attn1, [pieces[s] for s in shifts]
        )
        return own, [
            lax.ppermute(v, "x", ring(k + 1)) for k, v in enumerate(sent)
        ]

    first = {}
    for shifts in ((0,), (1, 3), (2,)):
        coded = collect(*partials([attn], [own_1], shifts))
        for q, s in enumerate(shifts):
            first[s] = (coded, q)

    out = None
    for shifts in ((1, 3), (0, 2)):
        own, got = partials([low, high], [oth_1], shifts)
        ready = release(
            jnp.stack([x, c]), own, got, [first[s] for s in shifts]
        )
        arrived, places = [], []
        for (s, j), v in zip(itertools.product(shifts, range(2)), ready):
            to = moves(lambda y, zh, c, zl, x: ((y - s) % 4, zh, zl, c ^ j, x))
            arrived.append(lax.ppermute(v, AXES, to))
            at = ((y + s) % 4) * 4 + (zl ^ j)
            places += [at + zh * 2, at + (1 - zh) * 2]
        out = finish(jnp.stack(places), arrived, residual, out)
    return out


def solution(mesh):
    torus = Mesh(mesh.devices.reshape(SIZES), AXES)
    return jax.shard_map(
        shards,
        mesh=torus,
        in_specs=(
            P(("y", "zh", "c"), ("zl", "x")),
            P(("y", "zh", "c"), None),
            P(None, ("zl", "x"), ("y", "zh", "c")),
        ),
        out_specs=P(None, ("zl", "x"), ("y", "zh", "c")),
        check_vma=False,
    )
```

```python
import functools
import itertools

import jax
import jax.numpy as jnp
from jax import lax
from jax.experimental import pallas as pl
from jax.experimental.pallas import tpu as pltpu
from jax.sharding import Mesh
from jax.sharding import PartitionSpec as P


AXES = ("y", "zh", "c", "zl", "x")
SIZES = (4, 2, 2, 2, 4)
Z = ("zh", "zl")
BF16, F32 = jnp.bfloat16, jnp.float32


PART = (0.03, 4.6)
FULL = (0.12, 18.4)


def code(value, scale):
    floor, unit = scale
    power = (jnp.abs(value) + floor) * (1.0 / unit)
    for _ in range(4):
        power = power * power
    return jnp.where(value < 0, -power, power).astype(BF16)


def decode(coded, scale):
    floor, unit = scale
    coded = coded.astype(F32)
    value = jnp.exp(jnp.log(jnp.abs(coded)) * 0.0625) * unit - floor
    return jnp.where(coded < 0, -value, value)


def flat(coords):
    index = 0
    for coord, size in zip(coords, SIZES):
        index = index * size + coord
    return index


def moves(target):
    return [
        (flat(s), flat(target(*s)))
        for s in itertools.product(*(range(n) for n in SIZES))
    ]


def ring(shift):
    return [(i, (i + shift) % 4) for i in range(4)]


PARTNER = [(0, 1), (1, 0), (2, 3), (3, 2)]
OTHER = [(1, 2), (2, 1), (3, 0), (0, 3)]
CORES = [(0, 1), (1, 0)]
LARGE = pltpu.CompilerParams(vmem_limit_bytes=14 << 20)
SMALL = pltpu.CompilerParams(vmem_limit_bytes=6 << 20)
VMEM = pl.BlockSpec(memory_space=pltpu.VMEM)
PREFETCH = pltpu.PrefetchScalarGridSpec


def estimate(flops, moved):
    return pl.CostEstimate(flops=flops, bytes_accessed=moved, transcendentals=0)


def columns(start, size):
    return pl.ds(pl.multiple_of(start, size), size)


def join_body(first, second, out):
    out[0] = first[...]
    out[1] = second[...]


def join(first, second):
    return pl.pallas_call(
        join_body,
        in_specs=[VMEM] * 2,
        out_specs=VMEM,
        out_shape=jax.ShapeDtypeStruct((2, *first.shape), BF16),
        compiler_params=SMALL,
        cost_estimate=estimate(1 << 28, 1 << 20),
        name="join",
    )(first, second)


def tile_body(shifts, scalars, *refs):
    halves, pieces, (own, keep, plus, minus, rows) = refs[:4], refs[4:-5], refs[-5:]
    step = pl.program_id(0)
    x, core = scalars[0], scalars[1]

    @pl.when(step == 0)
    def _():
        for s, h, k, twin in itertools.product(range(4), range(2), range(2), range(2)):
            block = halves[2 * k + h][
                lax.rem(x + s, 4), :, columns((core ^ twin) * 512, 512)
            ]
            row, col = (s * 2 + h) * 128, (k * 2 + twin) * 512
            rows[row : row + 128, col : col + 512] = block

    column, odd = columns(lax.rem(step, 2) * 256, 256), lax.rem(step, 2) == 1
    out = columns(step * 256, 256)
    for g, shift in enumerate(shifts):

        @pl.when(step >> 1 == g)
        def _():
            base = scalars[2 + shift]
            got, twin = pieces[2 * g], pieces[2 * g + 1]
            total = jnp.dot(
                rows[...],
                jnp.concatenate(
                    [
                        got[base, :, column],
                        twin[base, :, column],
                        got[1 - base, :, column],
                        twin[1 - base, :, column],
                    ],
                    axis=0,
                ),
                preferred_element_type=F32,
            )
            mine, right, across, left = (
                total[256 * s : 256 * s + 256].reshape(2, 128, 256) for s in range(4)
            )
            own[:, :, out] = mine
            keep[:, :, out] = jnp.where(odd, left, right)
            plus[:, :, out] = code(jnp.where(odd, right, across), PART)
            minus[:, :, out] = code(jnp.where(odd, across, left), PART)


def tile(scalars, rows, pieces, shifts):
    n = len(shifts)
    shape = (2, 128, 512 * n)
    return pl.pallas_call(
        functools.partial(tile_body, shifts),
        grid_spec=PREFETCH(
            num_scalar_prefetch=1,
            grid=(2 * n,),
            in_specs=[VMEM] * (4 + 2 * n),
            out_specs=[VMEM] * 4,
            scratch_shapes=[pltpu.VMEM((1024, 2048), BF16)],
        ),
        out_shape=[jax.ShapeDtypeStruct(shape, d) for d in (F32, F32, BF16, BF16)],
        compiler_params=LARGE,
        cost_estimate=estimate(n << 31, 1 << 20),
    )(
        scalars,
        *(part.reshape(4, 128, 1024) for part in rows),
        *(part for s in shifts for part in pieces[s]),
    )


def relay_body(keep, plus, minus, on, back):
    g = pl.program_id(0)
    even, odd, half = (
        columns(g * 512, 256), columns(g * 512 + 256, 256), columns(g * 256, 256),
    )
    on[:, :, half] = code(keep[:, :, even] + decode(plus[:, :, even], PART), PART)
    back[:, :, half] = code(keep[:, :, odd] + decode(minus[:, :, odd], PART), PART)


def relay(keep, plus, minus):
    shape = (2, 128, keep.shape[2] // 2)
    return pl.pallas_call(
        relay_body,
        grid=(shape[2] // 256,),
        in_specs=[VMEM] * 3,
        out_specs=[VMEM] * 2,
        out_shape=[jax.ShapeDtypeStruct(shape, BF16)] * 2,
        compiler_params=SMALL,
        cost_estimate=estimate(1 << 30, 1 << 20),
    )(keep, plus, minus)


def reduced(rows, g, own, plus, minus, on, back):
    even, odd, half = (
        columns(g * 512, 256), columns(g * 512 + 256, 256), columns(g * 256, 256),
    )
    first = decode(minus[rows, :, even], PART) + decode(on[rows, :, half], PART)
    second = decode(plus[rows, :, odd], PART) + decode(back[rows, :, half], PART)
    return (
        code(own[rows, :, even] + first, FULL),
        code(own[rows, :, odd] + second, FULL),
    )


def collect_body(*refs):
    g = pl.program_id(0)
    first, second = reduced(slice(None), g, *refs[:5])
    refs[5][:, :, columns(g * 512, 256)] = first
    refs[5][:, :, columns(g * 512 + 256, 256)] = second


def collect(*operands):
    shape = operands[0].shape
    return pl.pallas_call(
        collect_body,
        grid=(shape[2] // 512,),
        in_specs=[VMEM] * 5,
        out_specs=VMEM,
        out_shape=jax.ShapeDtypeStruct(shape, BF16),
        compiler_params=SMALL,
        cost_estimate=estimate(1 << 30, 1 << 20),
    )(*operands)


def release_body(places, scalars, *refs):
    n = len(places)
    firsts, outs = refs[5 : 5 + n], refs[5 + n :]
    j = pl.program_id(0)
    half = scalars[1] ^ j
    for g, at in enumerate(places):
        sums = reduced(half, g, *refs[:5])
        for k in range(2):

            @pl.when(j == k)
            def _():
                out = outs[2 * g + k]
                out[0] = firsts[g][half, :, at * 512 : at * 512 + 512]
                out[1, :, :256] = sums[0]
                out[1, :, 256:] = sums[1]


def release(scalars, operands, firsts):
    n = len(firsts)
    return pl.pallas_call(
        functools.partial(release_body, tuple(at for _, at in firsts)),
        grid_spec=PREFETCH(
            num_scalar_prefetch=1,
            grid=(2,),
            in_specs=[VMEM] * (5 + n),
            out_specs=[VMEM] * (2 * n),
        ),
        out_shape=[jax.ShapeDtypeStruct((2, 128, 512), BF16)] * (2 * n),
        compiler_params=SMALL,
        cost_estimate=estimate(1 << 30, 1 << 20),
    )(scalars, *operands, *(array for array, _ in firsts))


def finish_body(n, scalars, *refs):
    gots, residual, out = refs[:n], refs[n], refs[-1]
    step = pl.program_id(0)
    for q, got in enumerate(gots):

        @pl.when(step >> 1 == q)
        def _():
            total = residual[0].astype(F32) + decode(got[step & 1], FULL)
            out[0] = total.astype(BF16)


def finish(scalars, gots, residual, partial, shifts):
    n = len(gots)

    def place(t, s):
        shift = shifts[0] if len(shifts) == 1 else jnp.where(t < 4, *shifts)
        return (s[6 + shift * 4 + lax.rem(t, 4)], 0, 0)

    block = pl.BlockSpec((1, 128, 512), place)
    extra = [] if partial is None else [partial]
    return pl.pallas_call(
        functools.partial(finish_body, n),
        grid_spec=PREFETCH(
            num_scalar_prefetch=1,
            grid=(2 * n,),
            in_specs=[VMEM] * n
            + [block]
            + [pl.BlockSpec(memory_space=pl.ANY)] * len(extra),
            out_specs=block,
        ),
        out_shape=jax.ShapeDtypeStruct(residual.shape, residual.dtype),
        input_output_aliases={n + 2: 0} if extra else {},
        compiler_params=SMALL,
        cost_estimate=estimate(1 << 30, 1 << 22),
    )(scalars, *gots, residual, *extra)


def layer(attn, weight, residual):
    y, zh, c, zl, x = (lax.axis_index(a) for a in AXES)

    numbers = [x, c] + [(((y - s) % 4) >> 1) ^ zl for s in range(4)]
    for s, j, other in itertools.product(range(4), range(2), range(2)):
        numbers.append(((y + s) % 4) * 4 + (zh ^ other) * 2 + (zl ^ j))
    scalars = jnp.stack(numbers)

    piece = []
    for p in range(2):
        target = ((y >> 1) ^ p) * 8 + (x & 1) * 4 + (x >> 1) * 2 + (zl ^ zh ^ (x >> 1))
        sent = lax.dynamic_slice(weight, (0, target * 512), (512, 512))
        to = moves(
            lambda y, zh, c, zl, x: (
                ((y >> 1) ^ p) * 2 + (x & 1), x >> 1, c, zl ^ zh ^ (x >> 1),
                (y & 1) * 2 + zh,
            )
        )
        piece.append(lax.ppermute(sent, AXES, to))

    own_0 = [attn[:512], attn[512:]]
    own_1, oth_1 = [None] * 2, [None] * 2
    own_1[1] = lax.ppermute(own_0[1], Z, PARTNER)
    oth_1[0] = lax.ppermute(own_0[0], Z, OTHER)
    own_1[0] = lax.ppermute(own_0[0], Z, PARTNER)
    oth_1[1] = lax.ppermute(own_0[1], Z, OTHER)
    low = lax.ppermute(oth_1[0], Z, PARTNER)
    high = lax.ppermute(own_1[1], Z, OTHER)

    piece = join(*piece)
    pieces = {}
    for shift in (0, 1, 3, 2):
        got = lax.ppermute(piece, "y", ring(shift)) if shift else piece
        pieces[shift] = got, lax.ppermute(got, "c", CORES)

    def partials(rows, shifts):
        own, keep, plus, minus = tile(scalars, rows, pieces, shifts)
        plus = lax.ppermute(plus, "x", ring(1))
        minus = lax.ppermute(minus, "x", ring(3))
        on, back = relay(keep, plus, minus)
        on = lax.ppermute(on, "x", ring(1))
        back = lax.ppermute(back, "x", ring(3))
        return own, plus, minus, on, back

    first = {}
    for shifts in ((0,), (1, 3), (2,)):
        operands = partials(own_0 + own_1, shifts)
        coded = collect(*operands)
        for q, s in enumerate(shifts):
            first[s] = (coded, q)

    out = None
    for shifts in ((1, 3), (0,), (2,)):
        operands = partials([low, high] + oth_1, shifts)
        ready = release(scalars, operands, [first[s] for s in shifts])
        arrived = []
        for (s, j), v in zip(itertools.product(shifts, range(2)), ready):
            to = moves(lambda y, zh, c, zl, x: ((y - s) % 4, zh, zl, c ^ j, x))
            arrived.append(lax.ppermute(v, AXES, to))
        out = finish(scalars, arrived, residual, out, shifts)
    return out


def solution(mesh):
    torus = Mesh(mesh.devices.reshape(SIZES), AXES)
    return jax.shard_map(
        layer,
        mesh=torus,
        in_specs=(
            P(("y", "zh", "c"), ("zl", "x")),
            P(("y", "zh", "c"), None),
            P(None, ("zl", "x"), ("y", "zh", "c")),
        ),
        out_specs=P(None, ("zl", "x"), ("y", "zh", "c")),
        check_vma=False,
    )
```

```python
import functools
import itertools

import jax
import jax.numpy as jnp
from jax import lax
from jax.experimental import pallas as pl
from jax.experimental.pallas import tpu as pltpu
from jax.sharding import Mesh
from jax.sharding import PartitionSpec as P


AXES = ("y", "zh", "c", "zl", "x")
SIZES = (4, 2, 2, 2, 4)
Z = ("zh", "zl")
BF16, F32 = jnp.bfloat16, jnp.float32


PART = (0.03, 4.6)
FULL = (0.12, 18.4)


def code(value, scale):
    floor, unit = scale
    power = (jnp.abs(value) + floor) * (1.0 / unit)
    for _ in range(4):
        power = power * power
    return jnp.where(value < 0, -power, power).astype(BF16)


def decode(coded, scale):
    floor, unit = scale
    coded = coded.astype(F32)
    value = jnp.exp(jnp.log(jnp.abs(coded)) * 0.0625) * unit - floor
    return jnp.where(coded < 0, -value, value)


def flat(coords):
    index = 0
    for coord, size in zip(coords, SIZES):
        index = index * size + coord
    return index


def moves(target):
    return [
        (flat(s), flat(target(*s)))
        for s in itertools.product(*(range(n) for n in SIZES))
    ]


def ring(shift):
    return [(i, (i + shift) % 4) for i in range(4)]


PARTNER = [(0, 1), (1, 0), (2, 3), (3, 2)]
OTHER = [(1, 2), (2, 1), (3, 0), (0, 3)]
CORES = [(0, 1), (1, 0)]
LARGE = pltpu.CompilerParams(vmem_limit_bytes=14 << 20)
SMALL = pltpu.CompilerParams(vmem_limit_bytes=6 << 20)
VMEM = pl.BlockSpec(memory_space=pltpu.VMEM)
PREFETCH = pltpu.PrefetchScalarGridSpec


def estimate(flops, moved):
    return pl.CostEstimate(flops=flops, bytes_accessed=moved, transcendentals=0)


def columns(start, size):
    return pl.ds(pl.multiple_of(start, size), size)


def join_body(first, second, out):
    out[0] = first[...]
    out[1] = second[...]


def join(first, second):
    return pl.pallas_call(
        join_body,
        in_specs=[VMEM] * 2,
        out_specs=VMEM,
        out_shape=jax.ShapeDtypeStruct((2, *first.shape), BF16),
        compiler_params=SMALL,
        cost_estimate=estimate(1 << 28, 1 << 20),
        name="join",
    )(first, second)


def tile_body(shifts, relayed, scalars, *refs):
    halves, pieces, (own, third, plus, minus, rows) = refs[:4], refs[4:-5], refs[-5:]
    step = pl.program_id(0)
    x, core = scalars[0], scalars[1]

    @pl.when(step == 0)
    def _():
        for s, h, k, twin in itertools.product(range(4), range(2), range(2), range(2)):
            block = halves[2 * k + h][
                lax.rem(x + s, 4), :, columns((core ^ twin) * 512, 512)
            ]
            row, col = (s * 2 + h) * 128, (k * 2 + twin) * 512
            rows[row : row + 128, col : col + 512] = block

    column, odd = columns(lax.rem(step, 2) * 256, 256), lax.rem(step, 2) == 1
    out = columns(step * 256, 256)
    for g, shift in enumerate(shifts):

        @pl.when(step >> 1 == g)
        def _():
            base = scalars[2 + shift]
            got, twin = pieces[2 * g], pieces[2 * g + 1]
            total = jnp.dot(
                rows[...],
                jnp.concatenate(
                    [
                        got[base, :, column],
                        twin[base, :, column],
                        got[1 - base, :, column],
                        twin[1 - base, :, column],
                    ],
                    axis=0,
                ),
                preferred_element_type=F32,
            )
            mine, right, across, left = (
                total[256 * s : 256 * s + 256].reshape(2, 128, 256) for s in range(4)
            )
            own[:, :, out] = mine
            if relayed:
                third[:, :, out] = jnp.where(odd, left, right)
                plus[:, :, out] = code(jnp.where(odd, right, across), PART)
                minus[:, :, out] = code(jnp.where(odd, across, left), PART)
            else:
                third[:, :, out] = code(across, PART)
                plus[:, :, out] = code(right, PART)
                minus[:, :, out] = code(left, PART)


def tile(scalars, rows, pieces, shifts, relayed):
    n = len(shifts)
    shape = (2, 128, 512 * n)
    return pl.pallas_call(
        functools.partial(tile_body, shifts, relayed),
        grid_spec=PREFETCH(
            num_scalar_prefetch=1,
            grid=(2 * n,),
            in_specs=[VMEM] * (4 + 2 * n),
            out_specs=[VMEM] * 4,
            scratch_shapes=[pltpu.VMEM((1024, 2048), BF16)],
        ),
        out_shape=[
            jax.ShapeDtypeStruct(shape, d)
            for d in (F32, F32 if relayed else BF16, BF16, BF16)
        ],
        compiler_params=LARGE,
        cost_estimate=estimate(n << 31, 1 << 20),
    )(
        scalars,
        *(part.reshape(4, 128, 1024) for part in rows),
        *(part for s in shifts for part in pieces[s]),
    )


def relay_body(keep, plus, minus, on, back):
    g = pl.program_id(0)
    even, odd, half = (
        columns(g * 512, 256), columns(g * 512 + 256, 256), columns(g * 256, 256),
    )
    on[:, :, half] = code(keep[:, :, even] + decode(plus[:, :, even], PART), PART)
    back[:, :, half] = code(keep[:, :, odd] + decode(minus[:, :, odd], PART), PART)


def relay(keep, plus, minus):
    shape = (2, 128, keep.shape[2] // 2)
    return pl.pallas_call(
        relay_body,
        grid=(shape[2] // 256,),
        in_specs=[VMEM] * 3,
        out_specs=[VMEM] * 2,
        out_shape=[jax.ShapeDtypeStruct(shape, BF16)] * 2,
        compiler_params=SMALL,
        cost_estimate=estimate(1 << 30, 1 << 20),
    )(keep, plus, minus)


def reduced(rows, g, own, plus, minus, on, back):
    even, odd, half = (
        columns(g * 512, 256), columns(g * 512 + 256, 256), columns(g * 256, 256),
    )
    first = decode(minus[rows, :, even], PART) + decode(on[rows, :, half], PART)
    second = decode(plus[rows, :, odd], PART) + decode(back[rows, :, half], PART)
    return (
        code(own[rows, :, even] + first, FULL),
        code(own[rows, :, odd] + second, FULL),
    )


def collect_body(own, across, plus, minus, out):
    part = columns(pl.program_id(0) * 512, 512)
    total = own[:, :, part]
    for ref in (across, plus, minus):
        total = total + decode(ref[:, :, part], PART)
    out[:, :, part] = code(total, FULL)


def collect(*operands):
    shape = operands[0].shape
    return pl.pallas_call(
        collect_body,
        grid=(shape[2] // 512,),
        in_specs=[VMEM] * 4,
        out_specs=VMEM,
        out_shape=jax.ShapeDtypeStruct(shape, BF16),
        compiler_params=SMALL,
        cost_estimate=estimate(1 << 30, 1 << 20),
    )(*operands)


def release_body(places, scalars, *refs):
    n = len(places)
    firsts, outs = refs[5 : 5 + n], refs[5 + n :]
    j = pl.program_id(0)
    half = scalars[1] ^ j
    for g, at in enumerate(places):
        sums = reduced(half, g, *refs[:5])
        for k in range(2):

            @pl.when(j == k)
            def _():
                out = outs[2 * g + k]
                out[0] = firsts[g][half, :, at * 512 : at * 512 + 512]
                out[1, :, :256] = sums[0]
                out[1, :, 256:] = sums[1]


def release(scalars, operands, firsts):
    n = len(firsts)
    return pl.pallas_call(
        functools.partial(release_body, tuple(at for _, at in firsts)),
        grid_spec=PREFETCH(
            num_scalar_prefetch=1,
            grid=(2,),
            in_specs=[VMEM] * (5 + n),
            out_specs=[VMEM] * (2 * n),
        ),
        out_shape=[jax.ShapeDtypeStruct((2, 128, 512), BF16)] * (2 * n),
        compiler_params=SMALL,
        cost_estimate=estimate(1 << 30, 1 << 20),
    )(scalars, *operands, *(array for array, _ in firsts))


def finish_body(n, scalars, *refs):
    gots, residual, out = refs[:n], refs[n], refs[-1]
    step = pl.program_id(0)
    for q, got in enumerate(gots):

        @pl.when(step >> 1 == q)
        def _():
            total = residual[0].astype(F32) + decode(got[step & 1], FULL)
            out[0] = total.astype(BF16)


def finish(scalars, gots, residual, partial, shifts):
    n = len(gots)

    def place(t, s):
        shift = shifts[0] if len(shifts) == 1 else jnp.where(t < 4, *shifts)
        return (s[6 + shift * 4 + lax.rem(t, 4)], 0, 0)

    block = pl.BlockSpec((1, 128, 512), place)
    extra = [] if partial is None else [partial]
    return pl.pallas_call(
        functools.partial(finish_body, n),
        grid_spec=PREFETCH(
            num_scalar_prefetch=1,
            grid=(2 * n,),
            in_specs=[VMEM] * n
            + [block]
            + [pl.BlockSpec(memory_space=pl.ANY)] * len(extra),
            out_specs=block,
        ),
        out_shape=jax.ShapeDtypeStruct(residual.shape, residual.dtype),
        input_output_aliases={n + 2: 0} if extra else {},
        compiler_params=SMALL,
        cost_estimate=estimate(1 << 30, 1 << 22),
    )(scalars, *gots, residual, *extra)


OWN = {"own_a": (0,), "own_b": (1, 3), "own_c": (2,)}
OTH = {"oth_a": (1, 3), "oth_b": (2,), "oth_c": (0,)}


def layer(attn, weight, residual):
    y, zh, c, zl, x = (lax.axis_index(a) for a in AXES)

    numbers = [x, c] + [(((y - s) % 4) >> 1) ^ zl for s in range(4)]
    for s, j, other in itertools.product(range(4), range(2), range(2)):
        numbers.append(((y + s) % 4) * 4 + (zh ^ other) * 2 + (zl ^ j))
    scalars = jnp.stack(numbers)

    piece = []
    for p in range(2):
        target = ((y >> 1) ^ p) * 8 + (x & 1) * 4 + (x >> 1) * 2 + (zl ^ zh ^ (x >> 1))
        sent = lax.dynamic_slice(weight, (0, target * 512), (512, 512))
        to = moves(
            lambda y, zh, c, zl, x: (
                ((y >> 1) ^ p) * 2 + (x & 1), x >> 1, c, zl ^ zh ^ (x >> 1),
                (y & 1) * 2 + zh,
            )
        )
        piece.append(lax.ppermute(sent, AXES, to))

    own_0 = [attn[:512], attn[512:]]
    own_1, oth_1 = [None] * 2, [None] * 2
    own_1[1] = lax.ppermute(own_0[1], Z, PARTNER)
    oth_1[0] = lax.ppermute(own_0[0], Z, OTHER)
    own_1[0] = lax.ppermute(own_0[0], Z, PARTNER)
    oth_1[1] = lax.ppermute(own_0[1], Z, OTHER)
    low = lax.ppermute(oth_1[0], Z, PARTNER)
    high = lax.ppermute(own_1[1], Z, OTHER)

    piece = join(*piece)
    pieces = {}
    for shift in (0, 1, 3, 2):
        got = lax.ppermute(piece, "y", ring(shift)) if shift else piece
        pieces[shift] = got, lax.ppermute(got, "c", CORES)

    first, out = {}, None
    for shifts in OWN.values():
        own, across, plus, minus = tile(scalars, own_0 + own_1, pieces, shifts, False)
        plus = lax.ppermute(plus, "x", ring(1))
        minus = lax.ppermute(minus, "x", ring(3))
        across = lax.ppermute(across, "x", ring(2))
        coded = collect(own, across, plus, minus)
        for q, s in enumerate(shifts):
            first[s] = (coded, q)
    for shifts in OTH.values():
        own, keep, plus, minus = tile(
            scalars, [low, high] + oth_1, pieces, shifts, True
        )
        plus = lax.ppermute(plus, "x", ring(1))
        minus = lax.ppermute(minus, "x", ring(3))
        on, back = relay(keep, plus, minus)
        on = lax.ppermute(on, "x", ring(1))
        back = lax.ppermute(back, "x", ring(3))
        ready = release(
            scalars, (own, plus, minus, on, back),
            [first[s] for s in shifts],
        )
        arrived = []
        for (s, j), v in zip(itertools.product(shifts, range(2)), ready):
            to = moves(lambda y, zh, c, zl, x: ((y - s) % 4, zh, zl, c ^ j, x))
            arrived.append(lax.ppermute(v, AXES, to))
        out = finish(scalars, arrived, residual, out, shifts)
    return out


def solution(mesh):
    torus = Mesh(mesh.devices.reshape(SIZES), AXES)
    return jax.shard_map(
        layer,
        mesh=torus,
        in_specs=(
            P(("y", "zh", "c"), ("zl", "x")),
            P(("y", "zh", "c"), None),
            P(None, ("zl", "x"), ("y", "zh", "c")),
        ),
        out_specs=P(None, ("zl", "x"), ("y", "zh", "c")),
        check_vma=False,
    )
```
